32 devices in a mesh: gz: 16 (over z, y, x), gy: 2 (over core).
Axes of the slice: x: 2, y: 2, z: 4, core: 2. Of those that a mesh axis runs over, the one named last changes fastest.
Arguments:
- snapshots: float32 [48, 64, 128, 256], P(None, 'gz', 'gy'), may hold values from -6 to 6
- energies: float32 [48], replicated, may hold values from 0.3 to 3
- plane_weight: float32 [64], P('gz'), may hold values from 1 to 10
Outputs:
- modes: float32 [16, 64, 128, 256], P(None, 'gz', 'gy')
- basis: float32 [48, 16], replicated
The draws below stay inside these ranges and needn't reach their ends.
All inputs are finite; a program needn't handle non-finite values.
Results may differ from the reference program's by a relative error of at most 0.0003.
Values sent between devices are 32-bit elements; how exact they have to be, the bound alone decides.
A program may use at most 128 MiB of HBM per device.

```python
import math
import jax
import jax.numpy as jnp
from jax import lax

S = 48
MODES = 16
ITERS = 6
NXF = 256
NY = 128
NZ = 64


def block_levels(own_key, dims, pieces, low, high):
    gain = 1.0
    for position, shards_of in pieces:
        steps = jax.random.uniform(jax.random.fold_in(jax.random.fold_in(own_key, 6), position), (shards_of,), jnp.float32, low / len(pieces), high / len(pieces))
        gain = gain * jnp.repeat(jnp.exp(steps), dims[position] // shards_of).reshape((-1,) + (1,) * (len(dims) - 1 - position))
    return gain


def bell_draw(rng, dims, scale, limit, split=(), kind=jnp.bfloat16):
    loudness = block_levels(rng, dims, split, -0.22, 0.18) if split else 1.0
    entries = jax.random.normal(rng, dims, jnp.float32) * scale * loudness
    return jnp.minimum(jnp.maximum(entries, -limit), limit).astype(kind)


def setup_inputs(seed: int = 0) -> dict:
    key_list = jax.random.split(jax.random.key(seed), 4)
    return {
        "snapshots": bell_draw(key_list[0], (S, NZ, NY, NXF), 1.0, 6.0, ((1, 16), (2, 2)), jnp.float32),
        "energies": jnp.clip(jnp.exp(jax.random.uniform(key_list[1], (S,), jnp.float32, math.log(0.3), math.log(3.0))), 0.3, 3.0),
        "plane_weight": jnp.clip(jnp.exp(math.log(10.0) - 2.3025851 * jax.random.uniform(key_list[2], (NZ,), jnp.float32) ** block_levels(key_list[2], (NZ,), ((0, 16),), -0.2, 0.2)), 1.0, 10.0),
    }


def reference(snapshots, energies, plane_weight):
    scaled = snapshots * energies[:, None, None, None]
    filtered = 0.25 * jnp.roll(scaled, 1, axis=1) + 0.5 * scaled + 0.25 * jnp.roll(scaled, -1, axis=1)
    total = filtered.shape[1] * filtered.shape[2] * filtered.shape[3]

    def add_plane(index, gram):
        plane = lax.dynamic_index_in_dim(filtered, index, 1, keepdims=False).reshape(S, -1)
        weight = lax.dynamic_index_in_dim(plane_weight, index, 0, keepdims=False)
        return gram + jnp.dot(plane * weight, plane.T, precision=lax.Precision.HIGHEST)
    gram = lax.fori_loop(0, NZ, add_plane, jnp.zeros((S, S), jnp.float32)) / total
    basis = jnp.eye(S, dtype=jnp.float32)[:, :MODES]
    for step in range(ITERS):
        image = jnp.dot(gram, basis, precision=lax.Precision.HIGHEST)
        factor = jnp.linalg.cholesky(jnp.dot(image.T, image, precision=lax.Precision.HIGHEST))
        basis = jax.scipy.linalg.solve_triangular(factor, image.T, lower=True).T
    raw = jnp.dot(basis.T, filtered.reshape(S, -1), precision=lax.Precision.HIGHEST)
    raw = raw.reshape(MODES, NZ, NY, NXF)
    norms = lax.optimization_barrier(jnp.sum(raw * raw * plane_weight[None, :, None, None], axis=(1, 2, 3))) / total
    modes = raw / jnp.sqrt(norms)[:, None, None, None]
    return (modes, basis)
```

```python
import functools

import jax
import jax.numpy as jnp
from jax import lax
from jax.experimental import pallas as pl
from jax.experimental.pallas import tpu as pltpu
from jax.sharding import PartitionSpec as P

MODES = 16
ITERS = 6
CHUNK = 8
LANES = 128
MESH = pl.DeviceIdType.MESH
HIGHEST = lax.Precision.HIGHEST
NT = (((1,), (1,)), ((), ()))


def butterfly(index, bit):
    return index + bit - 2 * bit * lax.rem(lax.div(index, bit), 2)


def bits_of(count):
    return [1 << k for k in range(count.bit_length() - 1)]


def gram_kernel(
    gz_count, gy_count, total,
    snap_ref, energy_ref, weight_ref, split_ref, gram_ref,
    own, halo, split, sums, arrived, own_sem, halo_send, halo_recv, split_sem, sum_send, sum_recv,
):
    count, planes, rows, width = snap_ref.shape
    chunks = rows // CHUNK
    halves = width // LANES
    me = lax.axis_index("gz")
    core = lax.axis_index("gy")
    right = lax.rem(me + 1, gz_count)
    left = lax.rem(me + gz_count - 1, gz_count)

    loads = [
        pltpu.make_async_copy(
            snap_ref.at[:, z, :, pl.ds(h * LANES, LANES)], own.at[z, h], own_sem.at[z, h]
        )
        for z in range(planes)
        for h in range(halves)
    ]
    for load in loads:
        load.start()

    partners = [{"gy": butterfly(core, bit)} for bit in bits_of(gy_count)]
    partners += [{"gz": butterfly(me, bit)} for bit in bits_of(gz_count)]
    barrier = pltpu.get_barrier_semaphore()
    greeted = [{"gz": left}, {"gz": right}] + partners
    for device in greeted:
        pl.semaphore_signal(barrier, inc=1, device_id=device, device_id_type=MESH)
    pl.semaphore_wait(barrier, len(greeted))

    def halo_copy(side, chunk, h):
        span = pl.ds(pl.multiple_of(chunk * CHUNK, CHUNK), CHUNK)
        return pltpu.make_async_remote_copy(
            src_ref=snap_ref.at[
                :, planes - 1 if side == 0 else 0, span, pl.ds(h * LANES, LANES)
            ],
            dst_ref=halo.at[side, h, :, span],
            send_sem=halo_send.at[side, h, chunk],
            recv_sem=halo_recv.at[side, h, chunk],
            device_id={"gz": right if side == 0 else left},
            device_id_type=MESH,
        )

    def send(chunk, carry):
        for h in range(halves):
            halo_copy(0, chunk, h).start()
            halo_copy(1, chunk, h).start()
        return carry

    lax.fori_loop(0, chunks, send, 0)
    for load in loads:
        load.wait()

    energy = jnp.broadcast_to(energy_ref[...], (count, LANES))

    def flat(ref):
        return [ref.at[h].reshape(count * rows, LANES) for h in range(halves)]

    stack = [flat(halo.at[0])] + [flat(own.at[z]) for z in range(planes)] + [flat(halo.at[1])]

    def split_copy(z, chunk):
        span = pl.ds(chunk * CHUNK, CHUNK)
        return pltpu.make_async_copy(
            split.at[z, span], split_ref.at[z, span], split_sem.at[z, chunk]
        )

    def add_rows(z, chunk, acc):
        below, middle, above = stack[z : z + 3]
        for r in range(CHUNK):
            y = chunk * CHUNK + r
            line = pl.ds(y, count, stride=rows)
            pieces = [
                energy * (0.25 * (b[line, :] + a[line, :]) + 0.5 * m[line, :])
                for b, m, a in zip(below, middle, above)
            ]
            value = jnp.concatenate(pieces, axis=1)
            high = value.astype(jnp.bfloat16)
            low = (value - high.astype(jnp.float32)).astype(jnp.bfloat16)
            both = jnp.concatenate([high, low], axis=0)
            split[z, y] = both
            first = lax.dot_general(both, high, NT, preferred_element_type=jnp.float32)
            second = lax.dot_general(high, low, NT, preferred_element_type=jnp.float32)
            acc = acc + (first[:count] + (first[count:] + second))
        split_copy(z, chunk).start()
        return acc

    zero = jnp.zeros((count, count), jnp.float32)
    gram = zero
    for z in range(1, planes - 1):
        acc = lax.fori_loop(0, chunks, functools.partial(add_rows, z), zero)
        gram = gram + weight_ref[z] * acc

    def edge(chunk, carry):
        for h in range(halves):
            halo_copy(0, chunk, h).wait_recv()
        first = add_rows(0, chunk, carry[0])
        for h in range(halves):
            halo_copy(1, chunk, h).wait_recv()
        return first, add_rows(planes - 1, chunk, carry[1])

    first, last = lax.fori_loop(0, chunks, edge, (zero, zero))
    gram = (gram + weight_ref[0] * first + weight_ref[planes - 1] * last) / total

    for step, partner in enumerate(partners):
        sums[step] = gram
        copy = pltpu.make_async_remote_copy(
            src_ref=sums.at[step],
            dst_ref=arrived.at[step],
            send_sem=sum_send.at[step],
            recv_sem=sum_recv.at[step],
            device_id=partner,
            device_id_type=MESH,
        )
        copy.start()
        copy.wait()
        gram = gram + arrived[step]
    gram_ref[...] = gram

    def drain(chunk, carry):
        for h in range(halves):
            halo_copy(0, chunk, h).wait_send()
            halo_copy(1, chunk, h).wait_send()
        for z in range(planes):
            split_copy(z, chunk).wait()
        return carry

    lax.fori_loop(0, chunks, drain, 0)


def modes_kernel(gram_ref, split_ref, modes_ref, basis_ref, split, staged, in_sem, out_sem):
    planes, rows, _, width = split_ref.shape
    count = gram_ref.shape[0]
    parts = in_sem.shape[1]
    part = rows // parts
    halves = width // LANES

    def load(z, p):
        span = pl.ds(p * part, part)
        return pltpu.make_async_copy(split_ref.at[z, span], split.at[z, span], in_sem.at[z, p])

    def store(z, p, h):
        span = pl.ds(pl.multiple_of(p * part, part), part)
        return pltpu.make_async_copy(
            staged.at[z, h, :, span],
            modes_ref.at[:, z, span, pl.ds(h * LANES, LANES)],
            out_sem.at[z, h, p],
        )

    for z in range(planes):
        for p in range(parts):
            load(z, p).start()

    gram = gram_ref[...]
    row = lax.broadcasted_iota(jnp.int32, (MODES, 1), 0)
    diagonal = (
        lax.broadcasted_iota(jnp.int32, (MODES, MODES), 0)
        == lax.broadcasted_iota(jnp.int32, (MODES, MODES), 1)
    )

    def iterate(step, basis):
        image = jnp.dot(basis, gram, precision=HIGHEST, preferred_element_type=jnp.float32)
        square = lax.dot_general(
            image, image, NT, precision=HIGHEST, preferred_element_type=jnp.float32
        )
        for j in range(MODES - 1):
            inverse = 1.0 / square[j : j + 1, j : j + 1]
            ratio = jnp.where(row > j, square[:, j : j + 1] * inverse, 0.0)
            image = image - ratio * image[j : j + 1, :]
            square = square - ratio * square[j : j + 1, :]
        pivots = jnp.sum(jnp.where(diagonal, square, 0.0), axis=1, keepdims=True)
        return image / jnp.sqrt(pivots)

    start = (
        lax.broadcasted_iota(jnp.int32, (MODES, count), 0)
        == lax.broadcasted_iota(jnp.int32, (MODES, count), 1)
    ).astype(jnp.float32)
    basis = lax.fori_loop(0, ITERS, iterate, start)
    basis_ref[...] = basis.T
    projected = jnp.dot(basis, gram, precision=HIGHEST, preferred_element_type=jnp.float32)
    norms = jnp.sum(basis * projected, axis=1, keepdims=True)
    scaled = basis / jnp.sqrt(norms)
    high = scaled.astype(jnp.bfloat16)
    low = (scaled - high.astype(jnp.float32)).astype(jnp.bfloat16)
    both = jnp.concatenate([high, low], axis=0)

    for z in range(planes):
        flat = [staged.at[z, h].reshape(MODES * rows, LANES) for h in range(halves)]

        def do_part(p, carry):
            load(z, p).wait()

            def group(g, carry):
                for r in range(8):
                    y = p * part + g * 8 + r
                    first = jnp.dot(
                        both, split[z, y, :count], preferred_element_type=jnp.float32
                    )
                    second = jnp.dot(
                        high, split[z, y, count:], preferred_element_type=jnp.float32
                    )
                    raw = first[:MODES] + (first[MODES:] + second)
                    for h in range(halves):
                        flat[h][pl.ds(y, MODES, stride=rows), :] = raw[
                            :, h * LANES : (h + 1) * LANES
                        ]
                return carry

            lax.fori_loop(0, part // 8, group, 0)
            for h in range(halves):
                store(z, p, h).start()
            return carry

        lax.fori_loop(0, parts, do_part, 0)
    for z in range(planes):
        for p in range(parts):
            for h in range(halves):
                store(z, p, h).wait()


def local(gz_count, gy_count, snapshots, energies, plane_weight):
    count, planes, rows, width = snapshots.shape
    total = planes * gz_count * rows * gy_count * width
    chunks = rows // CHUNK
    halves = width // LANES
    steps = len(bits_of(gz_count)) + len(bits_of(gy_count))
    anywhere = pl.BlockSpec(memory_space=pl.ANY)
    vmem = pl.BlockSpec(memory_space=pltpu.VMEM)
    split, gram = pl.pallas_call(
        functools.partial(gram_kernel, gz_count, gy_count, total),
        name="exchange_and_gram",
        out_shape=(
            jax.ShapeDtypeStruct((planes, rows, 2 * count, width), jnp.bfloat16),
            jax.ShapeDtypeStruct((count, count), jnp.float32),
        ),
        in_specs=[anywhere, vmem, pl.BlockSpec(memory_space=pltpu.SMEM)],
        out_specs=(anywhere, vmem),
        scratch_shapes=[
            pltpu.VMEM((planes, halves, count, rows, LANES), jnp.float32),
            pltpu.VMEM((2, halves, count, rows, LANES), jnp.float32),
            pltpu.VMEM((planes, rows, 2 * count, width), jnp.bfloat16),
            pltpu.VMEM((steps, count, count), jnp.float32),
            pltpu.VMEM((steps, count, count), jnp.float32),
            pltpu.SemaphoreType.DMA((planes, halves)),
            pltpu.SemaphoreType.DMA((2, halves, chunks)),
            pltpu.SemaphoreType.DMA((2, halves, chunks)),
            pltpu.SemaphoreType.DMA((planes, chunks)),
            pltpu.SemaphoreType.DMA((steps,)),
            pltpu.SemaphoreType.DMA((steps,)),
        ],
        compiler_params=pltpu.CompilerParams(
            collective_id=0, has_side_effects=True, vmem_limit_bytes=60 * 1024 * 1024
        ),
    )(snapshots, energies[:, None], plane_weight)
    parts = 4
    modes, basis = pl.pallas_call(
        modes_kernel,
        name="basis_and_modes",
        out_shape=(
            jax.ShapeDtypeStruct((MODES, planes, rows, width), jnp.float32),
            jax.ShapeDtypeStruct((count, MODES), jnp.float32),
        ),
        in_specs=[vmem, anywhere],
        out_specs=(anywhere, vmem),
        scratch_shapes=[
            pltpu.VMEM((planes, rows, 2 * count, width), jnp.bfloat16),
            pltpu.VMEM((planes, halves, MODES, rows, LANES), jnp.float32),
            pltpu.SemaphoreType.DMA((planes, parts)),
            pltpu.SemaphoreType.DMA((planes, halves, parts)),
        ],
        compiler_params=pltpu.CompilerParams(vmem_limit_bytes=60 * 1024 * 1024),
    )(gram, split)
    return (modes, basis)


def solution(mesh):
    return jax.shard_map(
        functools.partial(local, mesh.shape["gz"], mesh.shape["gy"]),
        mesh=mesh,
        in_specs=(P(None, "gz", "gy", None), P(), P("gz")),
        out_specs=(P(None, "gz", "gy", None), P()),
        check_vma=False,
    )
```

```python
import functools

import jax
import jax.numpy as jnp
from jax import lax
from jax.experimental import pallas as pl
from jax.experimental.pallas import tpu as pltpu
from jax.sharding import PartitionSpec as P

MODES = 16
ITERS = 6
CHUNK = 8
LANES = 128
MESH = pl.DeviceIdType.MESH
HIGHEST = lax.Precision.HIGHEST
NT = (((1,), (1,)), ((), ()))


def near_size(count):
    size = 1
    while size * size < count:
        size *= 2
    return size if count % size == 0 else 1


def gram_kernel(
    gz_count, gy_count, total,
    snap_ref, energy_ref, weight_ref, split_ref, gram_ref,
    own, halo, split, near_sums, far_sums,
    own_sem, halo_send, halo_recv, split_sem, near_send, near_recv, far_send, far_recv,
):
    count, planes, rows, width = snap_ref.shape
    chunks = rows // CHUNK
    halves = width // LANES
    me = lax.axis_index("gz")
    core = lax.axis_index("gy")
    right = lax.rem(me + 1, gz_count)
    left = lax.rem(me + gz_count - 1, gz_count)

    loads = [
        pltpu.make_async_copy(
            snap_ref.at[:, z, :, pl.ds(h * LANES, LANES)], own.at[z, h], own_sem.at[z, h]
        )
        for z in range(planes)
        for h in range(halves)
    ]
    for load in loads:
        load.start()

    near = near_size(gz_count)
    far = gz_count // near
    inner = lax.rem(me, near)
    outer = lax.div(me, near)
    near_mine = inner * gy_count + core
    near_peers = []
    for k in range(1, near * gy_count):
        peer = lax.rem(near_mine + k, near * gy_count)
        place = outer * near + lax.div(peer, gy_count)
        near_peers.append({"gz": place, "gy": lax.rem(peer, gy_count)})
    far_peers = [{"gz": lax.rem(outer + k, far) * near + inner} for k in range(1, far)]
    partners = near_peers + far_peers
    barrier = pltpu.get_barrier_semaphore()
    greeted = [{"gz": left}, {"gz": right}] + partners
    for device in greeted:
        pl.semaphore_signal(barrier, inc=1, device_id=device, device_id_type=MESH)
    pl.semaphore_wait(barrier, len(greeted))

    def halo_copy(side, chunk, h):
        span = pl.ds(pl.multiple_of(chunk * CHUNK, CHUNK), CHUNK)
        return pltpu.make_async_remote_copy(
            src_ref=snap_ref.at[
                :, planes - 1 if side == 0 else 0, span, pl.ds(h * LANES, LANES)
            ],
            dst_ref=halo.at[side, h, :, span],
            send_sem=halo_send.at[side, h, chunk],
            recv_sem=halo_recv.at[side, h, chunk],
            device_id={"gz": right if side == 0 else left},
            device_id_type=MESH,
        )

    def send(chunk, carry):
        for h in range(halves):
            halo_copy(0, chunk, h).start()
            halo_copy(1, chunk, h).start()
        return carry

    lax.fori_loop(0, chunks, send, 0)
    for load in loads:
        load.wait()

    column = lax.broadcasted_iota(jnp.int32, (count, count), 0)
    lane = lax.broadcasted_iota(jnp.int32, (count, count), 1)
    spread = jnp.where(column == lane, jnp.broadcast_to(energy_ref[...], (count, count)), 0.0)
    energy = jnp.broadcast_to(jnp.sum(spread, axis=1, keepdims=True), (count, LANES))

    def flat(ref):
        return [ref.at[h].reshape(count * rows, LANES) for h in range(halves)]

    stack = [flat(halo.at[0])] + [flat(own.at[z]) for z in range(planes)] + [flat(halo.at[1])]

    def split_copy(z, chunk):
        span = pl.ds(chunk * CHUNK, CHUNK)
        return pltpu.make_async_copy(
            split.at[z, span], split_ref.at[z, span], split_sem.at[z, chunk]
        )

    def add_rows(z, chunk, acc):
        below, middle, above = stack[z : z + 3]
        for r in range(CHUNK):
            y = chunk * CHUNK + r
            line = pl.ds(y, count, stride=rows)
            pieces = [
                energy * (0.25 * (b[line, :] + a[line, :]) + 0.5 * m[line, :])
                for b, m, a in zip(below, middle, above)
            ]
            value = jnp.concatenate(pieces, axis=1)
            high = value.astype(jnp.bfloat16)
            low = (value - high.astype(jnp.float32)).astype(jnp.bfloat16)
            both = jnp.concatenate([high, low], axis=0)
            split[z, y] = both
            first = lax.dot_general(both, high, NT, preferred_element_type=jnp.float32)
            second = lax.dot_general(high, low, NT, preferred_element_type=jnp.float32)
            acc = acc + (first[:count] + (first[count:] + second))
        split_copy(z, chunk).start()
        return acc

    zero = jnp.zeros((count, count), jnp.float32)
    gram = zero
    for z in range(1, planes - 1):
        acc = lax.fori_loop(0, chunks, functools.partial(add_rows, z), zero)
        gram = gram + weight_ref[z] * acc

    def edge(chunk, carry):
        for h in range(halves):
            halo_copy(0, chunk, h).wait_recv()
        first = add_rows(0, chunk, carry[0])
        for h in range(halves):
            halo_copy(1, chunk, h).wait_recv()
        return first, add_rows(planes - 1, chunk, carry[1])

    first, last = lax.fori_loop(0, chunks, edge, (zero, zero))
    gram = (gram + weight_ref[0] * first + weight_ref[planes - 1] * last) / total

    def share(value, slots, mine, peers, send_sem, recv_sem):
        slots[mine] = value
        copies = [
            pltpu.make_async_remote_copy(
                src_ref=slots.at[mine],
                dst_ref=slots.at[mine],
                send_sem=send_sem.at[k],
                recv_sem=recv_sem.at[k],
                device_id=peer,
                device_id_type=MESH,
            )
            for k, peer in enumerate(peers)
        ]
        for copy in copies:
            copy.start()
        for copy in copies:
            copy.wait()
        return sum(slots[k] for k in range(1, slots.shape[0])) + slots[0]

    gram = share(gram, near_sums, near_mine, near_peers, near_send, near_recv)
    gram = share(gram, far_sums, outer, far_peers, far_send, far_recv)
    gram_ref[...] = gram

    def drain(chunk, carry):
        for h in range(halves):
            halo_copy(0, chunk, h).wait_send()
            halo_copy(1, chunk, h).wait_send()
        for z in range(planes):
            split_copy(z, chunk).wait()
        return carry

    lax.fori_loop(0, chunks, drain, 0)


def modes_kernel(gram_ref, split_ref, modes_ref, basis_ref, split, staged, in_sem, out_sem):
    planes, rows, _, width = split_ref.shape
    count = gram_ref.shape[0]
    parts = in_sem.shape[1]
    part = rows // parts
    halves = width // LANES

    def load(z, p):
        span = pl.ds(p * part, part)
        return pltpu.make_async_copy(split_ref.at[z, span], split.at[z, span], in_sem.at[z, p])

    def store(z, p, h):
        span = pl.ds(pl.multiple_of(p * part, part), part)
        return pltpu.make_async_copy(
            staged.at[z, h, :, span],
            modes_ref.at[:, z, span, pl.ds(h * LANES, LANES)],
            out_sem.at[z, h, p],
        )

    for z in range(planes):
        for p in range(parts):
            load(z, p).start()

    gram = gram_ref[...]
    row = lax.broadcasted_iota(jnp.int32, (MODES, count), 0)
    def iterate(step, basis):
        image = jnp.dot(basis, gram, precision=HIGHEST, preferred_element_type=jnp.float32)
        square = lax.dot_general(
            image, image, NT, precision=HIGHEST, preferred_element_type=jnp.float32
        )
        columns = [
            jnp.broadcast_to(square[:, j : j + 1], (MODES, count)) for j in range(MODES)
        ]
        scale = jnp.zeros((MODES, count), jnp.float32)
        for j in range(MODES):
            pivot = columns[j][j : j + 1, :]
            scale = jnp.where(row == j, pivot, scale)
            if j < MODES - 1:
                ratio = jnp.where(row > j, columns[j] * (1.0 / pivot), 0.0)
                for k in range(j + 1, MODES):
                    columns[k] = columns[k] - ratio * columns[k][j : j + 1, :]
                image = image - ratio * image[j : j + 1, :]
        return image / jnp.sqrt(scale)

    start = (
        lax.broadcasted_iota(jnp.int32, (MODES, count), 0)
        == lax.broadcasted_iota(jnp.int32, (MODES, count), 1)
    ).astype(jnp.float32)
    basis = lax.fori_loop(0, ITERS, iterate, start)
    basis_ref[...] = basis
    projected = jnp.dot(basis, gram, precision=HIGHEST, preferred_element_type=jnp.float32)
    norms = jnp.sum(basis * projected, axis=1, keepdims=True)
    scaled = basis / jnp.sqrt(norms)
    high = scaled.astype(jnp.bfloat16).astype(jnp.float32)
    top = jnp.concatenate([high, high], axis=1)
    bottom = jnp.concatenate([scaled - high, jnp.zeros_like(high)], axis=1)
    both = jnp.concatenate([top, bottom], axis=0).astype(jnp.bfloat16)

    for z in range(planes):
        flat = [staged.at[z, h].reshape(MODES * rows, LANES) for h in range(halves)]

        def do_part(p, carry):
            load(z, p).wait()

            for r in range(part):
                y = p * part + r
                pair = jnp.dot(both, split[z, y], preferred_element_type=jnp.float32)
                raw = pair[:MODES] + pair[MODES:]
                for h in range(halves):
                    flat[h][pl.ds(y, MODES, stride=rows), :] = raw[
                        :, h * LANES : (h + 1) * LANES
                    ]
            for h in range(halves):
                store(z, p, h).start()
            return carry

        lax.fori_loop(0, parts, do_part, 0)
    for z in range(planes):
        for p in range(parts):
            for h in range(halves):
                store(z, p, h).wait()


def local(gz_count, gy_count, snapshots, energies, plane_weight):
    count, planes, rows, width = snapshots.shape
    total = planes * gz_count * rows * gy_count * width
    chunks = rows // CHUNK
    halves = width // LANES
    near = near_size(gz_count)
    near_total = near * gy_count
    far = gz_count // near
    anywhere = pl.BlockSpec(memory_space=pl.ANY)
    vmem = pl.BlockSpec(memory_space=pltpu.VMEM)
    split, gram = pl.pallas_call(
        functools.partial(gram_kernel, gz_count, gy_count, total),
        name="exchange_and_gram",
        out_shape=(
            jax.ShapeDtypeStruct((planes, rows, 2 * count, width), jnp.bfloat16),
            jax.ShapeDtypeStruct((count, count), jnp.float32),
        ),
        in_specs=[anywhere, vmem, pl.BlockSpec(memory_space=pltpu.SMEM)],
        out_specs=(anywhere, vmem),
        scratch_shapes=[
            pltpu.VMEM((planes, halves, count, rows, LANES), jnp.float32),
            pltpu.VMEM((2, halves, count, rows, LANES), jnp.float32),
            pltpu.VMEM((planes, rows, 2 * count, width), jnp.bfloat16),
            pltpu.VMEM((near_total, count, count), jnp.float32),
            pltpu.VMEM((far, count, count), jnp.float32),
            pltpu.SemaphoreType.DMA((planes, halves)),
            pltpu.SemaphoreType.DMA((2, halves, chunks)),
            pltpu.SemaphoreType.DMA((2, halves, chunks)),
            pltpu.SemaphoreType.DMA((planes, chunks)),
            pltpu.SemaphoreType.DMA((near_total,)),
            pltpu.SemaphoreType.DMA((near_total,)),
            pltpu.SemaphoreType.DMA((far,)),
            pltpu.SemaphoreType.DMA((far,)),
        ],
        compiler_params=pltpu.CompilerParams(
            collective_id=0, has_side_effects=True, vmem_limit_bytes=60 * 1024 * 1024
        ),
    )(snapshots, energies[None], plane_weight)
    parts = 2
    modes, basis = pl.pallas_call(
        modes_kernel,
        name="basis_and_modes",
        out_shape=(
            jax.ShapeDtypeStruct((MODES, planes, rows, width), jnp.float32),
            jax.ShapeDtypeStruct((MODES, count), jnp.float32),
        ),
        in_specs=[vmem, anywhere],
        out_specs=(anywhere, vmem),
        scratch_shapes=[
            pltpu.VMEM((planes, rows, 2 * count, width), jnp.bfloat16),
            pltpu.VMEM((planes, halves, MODES, rows, LANES), jnp.float32),
            pltpu.SemaphoreType.DMA((planes, parts)),
            pltpu.SemaphoreType.DMA((planes, halves, parts)),
        ],
        compiler_params=pltpu.CompilerParams(vmem_limit_bytes=60 * 1024 * 1024),
    )(gram, split)
    return (modes, basis.T)


def solution(mesh):
    return jax.shard_map(
        functools.partial(local, mesh.shape["gz"], mesh.shape["gy"]),
        mesh=mesh,
        in_specs=(P(None, "gz", "gy", None), P(), P("gz")),
        out_specs=(P(None, "gz", "gy", None), P()),
        check_vma=False,
    )
```

```python
import functools

import jax
import jax.numpy as jnp
from jax import lax
from jax.experimental import pallas as pl
from jax.experimental.pallas import tpu as pltpu
from jax.sharding import PartitionSpec as P

MODES = 16
ITERS = 6
CHUNK = 8
LANES = 128
MESH = pl.DeviceIdType.MESH
HIGHEST = lax.Precision.HIGHEST
NT = (((1,), (1,)), ((), ()))


def near_size(count):
    size = 1
    while size * size < count:
        size *= 2
    return size if count % size == 0 else 1


def gram_kernel(
    gz_count, gy_count, total,
    snap_ref, energy_ref, weight_ref, split_ref, gram_ref,
    own, halo, split, near_sums, far_sums,
    own_sem, halo_send, halo_recv, split_sem, near_send, near_recv, far_send, far_recv,
):
    count, planes, rows, width = snap_ref.shape
    chunks = rows // CHUNK
    halves = width // LANES
    me = lax.axis_index("gz")
    core = lax.axis_index("gy")
    right = lax.rem(me + 1, gz_count)
    left = lax.rem(me + gz_count - 1, gz_count)

    loads = [
        pltpu.make_async_copy(
            snap_ref.at[:, z, :, pl.ds(h * LANES, LANES)], own.at[z, h], own_sem.at[z, h]
        )
        for z in range(planes)
        for h in range(halves)
    ]
    for load in loads:
        load.start()

    near = near_size(gz_count)
    far = gz_count // near
    inner = lax.rem(me, near)
    outer = lax.div(me, near)
    near_mine = inner * gy_count + core
    near_peers = []
    for k in range(1, near * gy_count):
        peer = lax.rem(near_mine + k, near * gy_count)
        place = outer * near + lax.div(peer, gy_count)
        near_peers.append({"gz": place, "gy": lax.rem(peer, gy_count)})
    far_peers = [{"gz": lax.rem(outer + k, far) * near + inner} for k in range(1, far)]
    partners = near_peers + far_peers
    barrier = pltpu.get_barrier_semaphore()
    greeted = [{"gz": left}, {"gz": right}] + partners
    for device in greeted:
        pl.semaphore_signal(barrier, inc=1, device_id=device, device_id_type=MESH)
    pl.semaphore_wait(barrier, len(greeted))

    def halo_copy(side, chunk, h):
        span = pl.ds(pl.multiple_of(chunk * CHUNK, CHUNK), CHUNK)
        return pltpu.make_async_remote_copy(
            src_ref=snap_ref.at[
                :, (1 - side) * (planes - 1), span, pl.ds(h * LANES, LANES)
            ],
            dst_ref=halo.at[side, h, :, span],
            send_sem=halo_send.at[side, h, chunk],
            recv_sem=halo_recv.at[side, h, chunk],
            device_id={"gz": lax.rem(me + 1 - 2 * side + gz_count, gz_count)},
            device_id_type=MESH,
        )

    def send(chunk, carry):
        for h in range(halves):
            halo_copy(1 - lax.rem(me, 2), chunk, h).start()
            halo_copy(lax.rem(me, 2), chunk, h).start()
        return carry

    lax.fori_loop(0, chunks, send, 0)
    for load in loads:
        load.wait()

    column = lax.broadcasted_iota(jnp.int32, (count, count), 0)
    lane = lax.broadcasted_iota(jnp.int32, (count, count), 1)
    spread = jnp.where(column == lane, jnp.broadcast_to(energy_ref[...], (count, count)), 0.0)
    energy = jnp.broadcast_to(jnp.sum(spread, axis=1, keepdims=True), (count, LANES))

    def flat(ref):
        return [ref.at[h].reshape(count * rows, LANES) for h in range(halves)]

    stack = [flat(halo.at[0])] + [flat(own.at[z]) for z in range(planes)] + [flat(halo.at[1])]

    def split_copy(z, chunk):
        span = pl.ds(chunk * CHUNK, CHUNK)
        return pltpu.make_async_copy(
            split.at[z, span], split_ref.at[z, span], split_sem.at[z, chunk]
        )

    def add_rows(z, chunk, acc, begin=0, end=halves):
        below, middle, above = stack[z : z + 3]
        for r in range(CHUNK):
            y = chunk * CHUNK + r
            line = pl.ds(y, count, stride=rows)
            pieces = [
                energy * (0.25 * (b[line, :] + a[line, :]) + 0.5 * m[line, :])
                for b, m, a in zip(below[begin:end], middle[begin:end], above[begin:end])
            ]
            value = jnp.concatenate(pieces, axis=1)
            high = value.astype(jnp.bfloat16)
            low = (value - high.astype(jnp.float32)).astype(jnp.bfloat16)
            both = jnp.concatenate([high, low], axis=0)
            split[z, y, :, begin * LANES : end * LANES] = both
            first = lax.dot_general(both, high, NT, preferred_element_type=jnp.float32)
            second = lax.dot_general(high, low, NT, preferred_element_type=jnp.float32)
            acc = acc + (first[:count] + (first[count:] + second))
        return acc

    def add_inner(z, chunk, acc):
        acc = add_rows(z, chunk, acc)
        split_copy(z, chunk).start()
        return acc

    zero = jnp.zeros((count, count), jnp.float32)
    gram = zero
    for z in range(1, planes - 1):
        acc = lax.fori_loop(0, chunks, functools.partial(add_inner, z), zero)
        gram = gram + weight_ref[z] * acc

    def edge(chunk, carry):
        first, last = carry
        for h in range(halves):
            halo_copy(0, chunk, h).wait_recv()
            first = add_rows(0, chunk, first, h, h + 1)
            halo_copy(1, chunk, h).wait_recv()
            last = add_rows(planes - 1, chunk, last, h, h + 1)
        split_copy(0, chunk).start()
        split_copy(planes - 1, chunk).start()
        return first, last

    first, last = lax.fori_loop(0, chunks, edge, (zero, zero))
    gram = (gram + weight_ref[0] * first + weight_ref[planes - 1] * last) / total

    def share(value, slots, mine, peers, send_sem, recv_sem):
        slots[mine] = value
        copies = [
            pltpu.make_async_remote_copy(
                src_ref=slots.at[mine],
                dst_ref=slots.at[mine],
                send_sem=send_sem.at[k],
                recv_sem=recv_sem.at[k],
                device_id=peer,
                device_id_type=MESH,
            )
            for k, peer in enumerate(peers)
        ]
        for copy in copies:
            copy.start()
        for copy in copies:
            copy.wait()
        return sum(slots[k] for k in range(1, slots.shape[0])) + slots[0]

    third = count // 3
    spare = near_sums.shape[2] - 2 * count
    packed = jnp.concatenate(
        [gram[k * third : (k + 1) * third, k * third :] for k in range(3)]
        + [jnp.zeros((third, spare), jnp.float32)],
        axis=1,
    )
    packed = share(packed, near_sums, near_mine, near_peers, near_send, near_recv)
    packed = share(packed, far_sums, outer, far_peers, far_send, far_recv)
    bands = [
        packed[:, :count],
        jnp.concatenate([zero[:third, :third], packed[:, count : 2 * count - third]], axis=1),
        jnp.concatenate(
            [zero[:third, : 2 * third], packed[:, 2 * count - third : 2 * count]], axis=1
        ),
    ]
    upper = jnp.concatenate(bands, axis=0)
    gram_ref[...] = jnp.where(column <= lane, upper, upper.T)

    def drain(chunk, carry):
        for h in range(halves):
            halo_copy(0, chunk, h).wait_send()
            halo_copy(1, chunk, h).wait_send()
        for z in range(planes):
            split_copy(z, chunk).wait()
        return carry

    lax.fori_loop(0, chunks, drain, 0)


def modes_kernel(gram_ref, split_ref, modes_ref, basis_ref, split, staged, in_sem, out_sem):
    planes, rows, _, width = split_ref.shape
    count = gram_ref.shape[0]
    parts = in_sem.shape[1]
    part = rows // parts
    halves = width // LANES

    def load(z, p):
        span = pl.ds(p * part, part)
        return pltpu.make_async_copy(split_ref.at[z, span], split.at[z, span], in_sem.at[z, p])

    def store(z, p, h):
        span = pl.ds(pl.multiple_of(p * part, part), part)
        return pltpu.make_async_copy(
            staged.at[z, h, :, span],
            modes_ref.at[:, z, span, pl.ds(h * LANES, LANES)],
            out_sem.at[z, h, p],
        )

    for z in range(planes):
        for p in range(parts):
            load(z, p).start()

    gram = gram_ref[...]
    row = lax.broadcasted_iota(jnp.int32, (MODES, count), 0)
    def iterate(step, basis):
        image = jnp.dot(basis, gram, precision=HIGHEST, preferred_element_type=jnp.float32)
        square = lax.dot_general(
            image, image, NT, precision=HIGHEST, preferred_element_type=jnp.float32
        )
        columns = [
            jnp.broadcast_to(square[:, j : j + 1], (MODES, count)) for j in range(MODES)
        ]
        scale = jnp.zeros((MODES, count), jnp.float32)
        for j in range(MODES):
            pivot = columns[j][j : j + 1, :]
            scale = jnp.where(row == j, pivot, scale)
            if j < MODES - 1:
                ratio = jnp.where(row > j, columns[j] * (1.0 / pivot), 0.0)
                for k in range(j + 1, MODES):
                    columns[k] = columns[k] - ratio * columns[k][j : j + 1, :]
                image = image - ratio * image[j : j + 1, :]
        return image / jnp.sqrt(scale)

    start = (
        lax.broadcasted_iota(jnp.int32, (MODES, count), 0)
        == lax.broadcasted_iota(jnp.int32, (MODES, count), 1)
    ).astype(jnp.float32)
    basis = lax.fori_loop(0, ITERS, iterate, start)
    basis_ref[...] = basis
    projected = jnp.dot(basis, gram, precision=HIGHEST, preferred_element_type=jnp.float32)
    norms = jnp.sum(basis * projected, axis=1, keepdims=True)
    scaled = basis / jnp.sqrt(norms)
    high = scaled.astype(jnp.bfloat16).astype(jnp.float32)
    top = jnp.concatenate([high, high], axis=1)
    bottom = jnp.concatenate([scaled - high, jnp.zeros_like(high)], axis=1)
    both = jnp.concatenate([top, bottom], axis=0).astype(jnp.bfloat16)

    for z in range(planes):
        flat = [staged.at[z, h].reshape(MODES * rows, LANES) for h in range(halves)]

        def do_part(p, carry):
            load(z, p).wait()

            for r in range(part):
                y = p * part + r
                pair = jnp.dot(both, split[z, y], preferred_element_type=jnp.float32)
                raw = pair[:MODES] + pair[MODES:]
                for h in range(halves):
                    flat[h][pl.ds(y, MODES, stride=rows), :] = raw[
                        :, h * LANES : (h + 1) * LANES
                    ]
            for h in range(halves):
                store(z, p, h).start()
            return carry

        lax.fori_loop(0, parts, do_part, 0)
    for z in range(planes):
        for p in range(parts):
            for h in range(halves):
                store(z, p, h).wait()


def local(gz_count, gy_count, snapshots, energies, plane_weight):
    count, planes, rows, width = snapshots.shape
    total = planes * gz_count * rows * gy_count * width
    chunks = rows // CHUNK
    halves = width // LANES
    near = near_size(gz_count)
    near_total = near * gy_count
    far = gz_count // near
    anywhere = pl.BlockSpec(memory_space=pl.ANY)
    vmem = pl.BlockSpec(memory_space=pltpu.VMEM)
    split, gram = pl.pallas_call(
        functools.partial(gram_kernel, gz_count, gy_count, total),
        name="exchange_and_gram",
        out_shape=(
            jax.ShapeDtypeStruct((planes, rows, 2 * count, width), jnp.bfloat16),
            jax.ShapeDtypeStruct((count, count), jnp.float32),
        ),
        in_specs=[anywhere, vmem, pl.BlockSpec(memory_space=pltpu.SMEM)],
        out_specs=(anywhere, vmem),
        scratch_shapes=[
            pltpu.VMEM((planes, halves, count, rows, LANES), jnp.float32),
            pltpu.VMEM((2, halves, count, rows, LANES), jnp.float32),
            pltpu.VMEM((planes, rows, 2 * count, width), jnp.bfloat16),
            pltpu.VMEM((near_total, count // 3, LANES), jnp.float32),
            pltpu.VMEM((far, count // 3, LANES), jnp.float32),
            pltpu.SemaphoreType.DMA((planes, halves)),
            pltpu.SemaphoreType.DMA((2, halves, chunks)),
            pltpu.SemaphoreType.DMA((2, halves, chunks)),
            pltpu.SemaphoreType.DMA((planes, chunks)),
            pltpu.SemaphoreType.DMA((near_total,)),
            pltpu.SemaphoreType.DMA((near_total,)),
            pltpu.SemaphoreType.DMA((far,)),
            pltpu.SemaphoreType.DMA((far,)),
        ],
        compiler_params=pltpu.CompilerParams(
            collective_id=0, has_side_effects=True, vmem_limit_bytes=60 * 1024 * 1024
        ),
    )(snapshots, energies[None], plane_weight)
    parts = 2
    modes, basis = pl.pallas_call(
        modes_kernel,
        name="basis_and_modes",
        out_shape=(
            jax.ShapeDtypeStruct((MODES, planes, rows, width), jnp.float32),
            jax.ShapeDtypeStruct((MODES, count), jnp.float32),
        ),
        in_specs=[vmem, anywhere],
        out_specs=(anywhere, vmem),
        scratch_shapes=[
            pltpu.VMEM((planes, rows, 2 * count, width), jnp.bfloat16),
            pltpu.VMEM((planes, halves, MODES, rows, LANES), jnp.float32),
            pltpu.SemaphoreType.DMA((planes, parts)),
            pltpu.SemaphoreType.DMA((planes, halves, parts)),
        ],
        compiler_params=pltpu.CompilerParams(vmem_limit_bytes=60 * 1024 * 1024),
    )(gram, split)
    return (modes, basis.T)


def solution(mesh):
    return jax.shard_map(
        functools.partial(local, mesh.shape["gz"], mesh.shape["gy"]),
        mesh=mesh,
        in_specs=(P(None, "gz", "gy", None), P(), P("gz")),
        out_specs=(P(None, "gz", "gy", None), P()),
        check_vma=False,
    )
```

```python
import functools

import jax
import jax.numpy as jnp
from jax import lax
from jax.experimental import pallas as pl
from jax.experimental.pallas import tpu as pltpu
from jax.sharding import PartitionSpec as P

MODES = 16
ITERS = 6
CHUNK = 8
LANES = 128
MESH = pl.DeviceIdType.MESH
HIGHEST = lax.Precision.HIGHEST
NT = (((1,), (1,)), ((), ()))


def near_size(count):
    size = 1
    while size * size < count:
        size *= 2
    return size if count % size == 0 else 1


def gram_kernel(
    gz_count, gy_count, total,
    snap_ref, energy_ref, weight_ref, split_ref, gram_ref,
    own, halo, split, near_sums, far_sums,
    own_sem, halo_send, halo_recv, split_sem, near_send, near_recv, far_send, far_recv,
):
    count, planes, rows, width = snap_ref.shape
    chunks = rows // CHUNK
    halves = width // LANES
    me = lax.axis_index("gz")
    core = lax.axis_index("gy")
    right = lax.rem(me + 1, gz_count)
    left = lax.rem(me + gz_count - 1, gz_count)

    loads = [
        pltpu.make_async_copy(
            snap_ref.at[:, z, :, pl.ds(h * LANES, LANES)], own.at[z, h], own_sem.at[z, h]
        )
        for z in range(planes)
        for h in range(halves)
    ]
    for load in loads:
        load.start()

    near = near_size(gz_count)
    far = gz_count // near
    inner = lax.rem(me, near)
    outer = lax.div(me, near)
    near_mine = inner * gy_count + core
    near_peers = []
    for k in range(1, near * gy_count):
        peer = lax.rem(near_mine + k, near * gy_count)
        place = outer * near + lax.div(peer, gy_count)
        near_peers.append({"gz": place, "gy": lax.rem(peer, gy_count)})
    far_peers = [{"gz": lax.rem(outer + k, far) * near + inner} for k in range(1, far)]
    partners = near_peers + far_peers
    barrier = pltpu.get_barrier_semaphore()
    greeted = [{"gz": left}, {"gz": right}] + partners
    for device in greeted:
        pl.semaphore_signal(barrier, inc=1, device_id=device, device_id_type=MESH)
    pl.semaphore_wait(barrier, len(greeted))

    def halo_copy(side, chunk, h):
        span = pl.ds(pl.multiple_of(chunk * CHUNK, CHUNK), CHUNK)
        return pltpu.make_async_remote_copy(
            src_ref=snap_ref.at[
                :, (1 - side) * (planes - 1), span, pl.ds(h * LANES, LANES)
            ],
            dst_ref=halo.at[side, h, :, span],
            send_sem=halo_send.at[side, h, chunk],
            recv_sem=halo_recv.at[side, h, chunk],
            device_id={"gz": lax.rem(me + 1 - 2 * side + gz_count, gz_count)},
            device_id_type=MESH,
        )

    def send(step, carry):
        side = lax.rem(me + 1 + lax.div(step, chunks), 2)
        for h in range(halves):
            halo_copy(side, lax.rem(step, chunks), h).start()
        return carry

    lax.fori_loop(0, 2 * chunks, send, 0)
    for load in loads:
        load.wait()

    column = lax.broadcasted_iota(jnp.int32, (count, count), 0)
    lane = lax.broadcasted_iota(jnp.int32, (count, count), 1)
    spread = jnp.where(column == lane, jnp.broadcast_to(energy_ref[...], (count, count)), 0.0)
    energy = jnp.broadcast_to(jnp.sum(spread, axis=1, keepdims=True), (count, LANES))

    def flat(ref):
        return [ref.at[h].reshape(count * rows, LANES) for h in range(halves)]

    stack = [flat(halo.at[0])] + [flat(own.at[z]) for z in range(planes)] + [flat(halo.at[1])]

    def split_copy(z, chunk):
        span = pl.ds(chunk * CHUNK, CHUNK)
        return pltpu.make_async_copy(
            split.at[z, span], split_ref.at[z, span], split_sem.at[z, chunk]
        )

    def add_rows(z, chunk, acc, begin=0, end=halves):
        below, middle, above = stack[z : z + 3]
        for r in range(CHUNK):
            y = chunk * CHUNK + r
            line = pl.ds(y, count, stride=rows)
            pieces = [
                energy * (0.25 * (b[line, :] + a[line, :]) + 0.5 * m[line, :])
                for b, m, a in zip(below[begin:end], middle[begin:end], above[begin:end])
            ]
            value = jnp.concatenate(pieces, axis=1)
            high = value.astype(jnp.bfloat16)
            low = (value - high.astype(jnp.float32)).astype(jnp.bfloat16)
            both = jnp.concatenate([high, low], axis=0)
            split[z, y, :, begin * LANES : end * LANES] = both
            first = lax.dot_general(both, high, NT, preferred_element_type=jnp.float32)
            second = lax.dot_general(high, low, NT, preferred_element_type=jnp.float32)
            acc = acc + (first[:count] + (first[count:] + second))
        return acc

    def add_inner(z, chunk, acc):
        acc = add_rows(z, chunk, acc)
        split_copy(z, chunk).start()
        return acc

    zero = jnp.zeros((count, count), jnp.float32)
    gram = zero
    for z in range(1, planes - 1):
        acc = lax.fori_loop(0, chunks, functools.partial(add_inner, z), zero)
        gram = gram + weight_ref[z] * acc

    def edge(chunk, carry):
        first, last = carry
        for h in range(halves):
            halo_copy(0, chunk, h).wait_recv()
            first = add_rows(0, chunk, first, h, h + 1)
            halo_copy(1, chunk, h).wait_recv()
            last = add_rows(planes - 1, chunk, last, h, h + 1)
        split_copy(0, chunk).start()
        split_copy(planes - 1, chunk).start()
        return first, last

    first, last = lax.fori_loop(0, chunks, edge, (zero, zero))
    gram = (gram + weight_ref[0] * first + weight_ref[planes - 1] * last) / total

    def share(value, slots, mine, peers, send_sem, recv_sem):
        slots[mine] = value
        copies = [
            pltpu.make_async_remote_copy(
                src_ref=slots.at[mine],
                dst_ref=slots.at[mine],
                send_sem=send_sem.at[k],
                recv_sem=recv_sem.at[k],
                device_id=peer,
                device_id_type=MESH,
            )
            for k, peer in enumerate(peers)
        ]
        for copy in copies:
            copy.start()
        for copy in copies:
            copy.wait()
        return sum(slots[k] for k in range(1, slots.shape[0])) + slots[0]

    third = count // 3
    spare = near_sums.shape[2] - 2 * count
    packed = jnp.concatenate(
        [gram[k * third : (k + 1) * third, k * third :] for k in range(3)]
        + [jnp.zeros((third, spare), jnp.float32)],
        axis=1,
    )
    packed = share(packed, near_sums, near_mine, near_peers, near_send, near_recv)
    packed = share(packed, far_sums, outer, far_peers, far_send, far_recv)
    bands = [
        packed[:, :count],
        jnp.concatenate([zero[:third, :third], packed[:, count : 2 * count - third]], axis=1),
        jnp.concatenate(
            [zero[:third, : 2 * third], packed[:, 2 * count - third : 2 * count]], axis=1
        ),
    ]
    upper = jnp.concatenate(bands, axis=0)
    gram_ref[...] = jnp.where(column <= lane, upper, upper.T)

    def drain(chunk, carry):
        for h in range(halves):
            halo_copy(0, chunk, h).wait_send()
            halo_copy(1, chunk, h).wait_send()
        for z in range(planes):
            split_copy(z, chunk).wait()
        return carry

    lax.fori_loop(0, chunks, drain, 0)


def modes_kernel(gram_ref, split_ref, modes_ref, basis_ref, split, staged, in_sem, out_sem):
    planes, rows, _, width = split_ref.shape
    count = gram_ref.shape[0]
    parts = in_sem.shape[1]
    part = rows // parts
    halves = width // LANES

    def load(z, p):
        span = pl.ds(p * part, part)
        return pltpu.make_async_copy(split_ref.at[z, span], split.at[z, span], in_sem.at[z, p])

    def store(z, p, h):
        span = pl.ds(pl.multiple_of(p * part, part), part)
        return pltpu.make_async_copy(
            staged.at[z, h, :, span],
            modes_ref.at[:, z, span, pl.ds(h * LANES, LANES)],
            out_sem.at[z, h, p],
        )

    for z in range(planes):
        for p in range(parts):
            load(z, p).start()

    gram = gram_ref[...]
    row = lax.broadcasted_iota(jnp.int32, (MODES, count), 0)
    def iterate(step, basis):
        image = jnp.dot(basis, gram, precision=HIGHEST, preferred_element_type=jnp.float32)
        square = lax.dot_general(
            image, image, NT, precision=HIGHEST, preferred_element_type=jnp.float32
        )
        columns = [
            jnp.broadcast_to(square[:, j : j + 1], (MODES, count)) for j in range(MODES)
        ]
        scale = jnp.zeros((MODES, count), jnp.float32)
        for j in range(MODES):
            pivot = columns[j][j : j + 1, :]
            scale = jnp.where(row == j, pivot, scale)
            if j < MODES - 1:
                ratio = jnp.where(row > j, columns[j] * (1.0 / pivot), 0.0)
                for k in range(j + 1, MODES):
                    columns[k] = columns[k] - ratio * columns[k][j : j + 1, :]
                image = image - ratio * image[j : j + 1, :]
        return image / jnp.sqrt(scale)

    start = (
        lax.broadcasted_iota(jnp.int32, (MODES, count), 0)
        == lax.broadcasted_iota(jnp.int32, (MODES, count), 1)
    ).astype(jnp.float32)
    basis = lax.fori_loop(0, ITERS, iterate, start)
    basis_ref[...] = basis
    projected = jnp.dot(basis, gram, precision=HIGHEST, preferred_element_type=jnp.float32)
    norms = jnp.sum(basis * projected, axis=1, keepdims=True)
    scaled = basis / jnp.sqrt(norms)
    high = scaled.astype(jnp.bfloat16).astype(jnp.float32)
    top = jnp.concatenate([high, high], axis=1)
    bottom = jnp.concatenate([scaled - high, jnp.zeros_like(high)], axis=1)
    both = jnp.concatenate([top, bottom], axis=0).astype(jnp.bfloat16)

    for z in range(planes):
        flat = [staged.at[z, h].reshape(MODES * rows, LANES) for h in range(halves)]

        def do_part(p, carry):
            load(z, p).wait()

            for r in range(part):
                y = p * part + r
                pair = jnp.dot(both, split[z, y], preferred_element_type=jnp.float32)
                raw = pair[:MODES] + pair[MODES:]
                for h in range(halves):
                    flat[h][pl.ds(y, MODES, stride=rows), :] = raw[
                        :, h * LANES : (h + 1) * LANES
                    ]
            for h in range(halves):
                store(z, p, h).start()
            return carry

        lax.fori_loop(0, parts, do_part, 0)
    for z in range(planes):
        for p in range(parts):
            for h in range(halves):
                store(z, p, h).wait()


def local(gz_count, gy_count, snapshots, energies, plane_weight):
    count, planes, rows, width = snapshots.shape
    total = planes * gz_count * rows * gy_count * width
    chunks = rows // CHUNK
    halves = width // LANES
    near = near_size(gz_count)
    near_total = near * gy_count
    far = gz_count // near
    anywhere = pl.BlockSpec(memory_space=pl.ANY)
    vmem = pl.BlockSpec(memory_space=pltpu.VMEM)
    split, gram = pl.pallas_call(
        functools.partial(gram_kernel, gz_count, gy_count, total),
        name="exchange_and_gram",
        out_shape=(
            jax.ShapeDtypeStruct((planes, rows, 2 * count, width), jnp.bfloat16),
            jax.ShapeDtypeStruct((count, count), jnp.float32),
        ),
        in_specs=[anywhere, vmem, pl.BlockSpec(memory_space=pltpu.SMEM)],
        out_specs=(anywhere, vmem),
        scratch_shapes=[
            pltpu.VMEM((planes, halves, count, rows, LANES), jnp.float32),
            pltpu.VMEM((2, halves, count, rows, LANES), jnp.float32),
            pltpu.VMEM((planes, rows, 2 * count, width), jnp.bfloat16),
            pltpu.VMEM((near_total, count // 3, LANES), jnp.float32),
            pltpu.VMEM((far, count // 3, LANES), jnp.float32),
            pltpu.SemaphoreType.DMA((planes, halves)),
            pltpu.SemaphoreType.DMA((2, halves, chunks)),
            pltpu.SemaphoreType.DMA((2, halves, chunks)),
            pltpu.SemaphoreType.DMA((planes, chunks)),
            pltpu.SemaphoreType.DMA((near_total,)),
            pltpu.SemaphoreType.DMA((near_total,)),
            pltpu.SemaphoreType.DMA((far,)),
            pltpu.SemaphoreType.DMA((far,)),
        ],
        compiler_params=pltpu.CompilerParams(
            collective_id=0, has_side_effects=True, vmem_limit_bytes=60 * 1024 * 1024
        ),
    )(snapshots, energies[None], plane_weight)
    parts = 2
    modes, basis = pl.pallas_call(
        modes_kernel,
        name="basis_and_modes",
        out_shape=(
            jax.ShapeDtypeStruct((MODES, planes, rows, width), jnp.float32),
            jax.ShapeDtypeStruct((MODES, count), jnp.float32),
        ),
        in_specs=[vmem, anywhere],
        out_specs=(anywhere, vmem),
        scratch_shapes=[
            pltpu.VMEM((planes, rows, 2 * count, width), jnp.bfloat16),
            pltpu.VMEM((planes, halves, MODES, rows, LANES), jnp.float32),
            pltpu.SemaphoreType.DMA((planes, parts)),
            pltpu.SemaphoreType.DMA((planes, halves, parts)),
        ],
        compiler_params=pltpu.CompilerParams(vmem_limit_bytes=60 * 1024 * 1024),
    )(gram, split)
    return (modes, basis.T)


def solution(mesh):
    return jax.shard_map(
        functools.partial(local, mesh.shape["gz"], mesh.shape["gy"]),
        mesh=mesh,
        in_specs=(P(None, "gz", "gy", None), P(), P("gz")),
        out_specs=(P(None, "gz", "gy", None), P()),
        check_vma=False,
    )
```
